16 devices in a mesh: rep: 4 (over z, y), data: 4 (over x, core).
Axes of the slice: x: 2, y: 2, z: 2, core: 2. Of those that a mesh axis runs over, the one named last changes fastest.
Arguments:
- x: bfloat16 [2048, 5120], P(('rep', 'data')), parts along dimension 0
- adapter_id: int32 [2048], P(('rep', 'data')), parts along dimension 0
- dout: bfloat16 [2048, 5120], P(('rep', 'data')), parts along dimension 0
- w_gate: bfloat16 [5120, 13824], replicated
- w_up: bfloat16 [5120, 13824], replicated
- w_down: bfloat16 [13824, 5120], replicated
- a_gate: bfloat16 [64, 5120, 16], P('data')
- b_gate: bfloat16 [64, 16, 13824], P('data')
- a_up: bfloat16 [64, 5120, 16], P('data')
- b_up: bfloat16 [64, 16, 13824], P('data')
- a_down: bfloat16 [64, 13824, 16], P('data')
- b_down: bfloat16 [64, 16, 5120], P('data')
Outputs:
- output 1: bfloat16 [2048, 5120], P(('rep', 'data')), parts along dimension 0
- output 2: bfloat16 [2048, 5120], P(('rep', 'data')), parts along dimension 0
- output 3: float32 [256, 5120, 16], P(('rep', 'data')), parts along dimension 0
- output 4: float32 [256, 16, 13824], P(('rep', 'data')), parts along dimension 0
- output 5: float32 [256, 5120, 16], P(('rep', 'data')), parts along dimension 0
- output 6: float32 [256, 16, 13824], P(('rep', 'data')), parts along dimension 0
- output 7: float32 [256, 13824, 16], P(('rep', 'data')), parts along dimension 0
- output 8: float32 [256, 16, 5120], P(('rep', 'data')), parts along dimension 0
There are 4 independent parts. The reference program is written for one: setup_inputs(seed, part) draws one part's arguments, and reference() takes and returns one part's arrays. A program takes and returns all parts, laid end to end along the dimension named above; an argument that names none is the same for every part.
All inputs are finite; a program needn't handle non-finite values.
Results may differ from the reference program's by a relative error of at most 0.00763854.
Values are sent between devices in bfloat16 or wider.
A program may use at most 2 GiB of HBM per device.

```python
import jax
import jax.numpy as jnp
from jax import lax

TOKENS = 128
ADAPTERS = 16
MODEL_DIM = 5120
HIDDEN_DIM = 13824
LORA_RANK = 16
GROUP_SIZE = 4
CAPACITY = 96
LORA_ALPHA = 32
BLOCK_ROWS = 32

PART_TOKENS = TOKENS * GROUP_SIZE
NUM_ADAPTERS = ADAPTERS * GROUP_SIZE
LORA_SCALE = LORA_ALPHA / LORA_RANK


def draw_ids(rand_key):
    key_hot, key_off, key_shift, key_perm = jax.random.split(rand_key, 4)
    hot_owner = jax.random.randint(key_hot, (), 0, GROUP_SIZE)
    start_offset = jax.random.randint(key_off, (), 0, GROUP_SIZE - 1)
    owner_shift = jax.random.randint(key_shift, (GROUP_SIZE,), 0, ADAPTERS)
    spare_rows = TOKENS - CAPACITY
    source_dev = jnp.arange(GROUP_SIZE)[:, None]
    column_idx = jnp.arange(TOKENS)[None, :]
    hot_mask = column_idx < CAPACITY
    hot_local = (source_dev * CAPACITY + column_idx + owner_shift[hot_owner]) % ADAPTERS
    flat_index = start_offset + source_dev * spare_rows + column_idx - CAPACITY
    other_owner = (hot_owner + 1 + flat_index % (GROUP_SIZE - 1)) % GROUP_SIZE
    visit_count = flat_index // (GROUP_SIZE - 1)
    other_local = (visit_count + owner_shift[other_owner]) % ADAPTERS
    owner_ids = jnp.where(hot_mask, hot_owner, other_owner)
    local_ids = jnp.where(hot_mask, hot_local, other_local)
    id_table = owner_ids * ADAPTERS + local_ids
    perm_keys = jax.random.split(key_perm, GROUP_SIZE)
    perm_rows = jax.vmap(lambda perm_key: jax.random.permutation(perm_key, TOKENS))(perm_keys)
    id_table = jnp.take_along_axis(id_table, perm_rows, axis=1)
    return id_table.reshape(-1).astype(jnp.int32)


def normal_bf16(key_one, arr_shape, spread):
    return (jax.random.normal(key_one, arr_shape, jnp.float32) * spread).astype(jnp.bfloat16)


def setup_inputs(seed: int = 0, part: int = 0) -> dict:
    base_key = jax.random.key(seed)
    part_key = jax.random.fold_in(base_key, part)
    shared_keys = jax.random.split(base_key, 9)
    part_keys = jax.random.split(part_key, 3)
    b_std = 0.3 * LORA_RANK ** -0.5 / LORA_SCALE
    d_std = MODEL_DIM ** -0.5
    f_std = HIDDEN_DIM ** -0.5
    return {
        'x': normal_bf16(part_keys[0], (PART_TOKENS, MODEL_DIM), 1.0),
        'adapter_id': draw_ids(part_keys[1]),
        'dout': normal_bf16(part_keys[2], (PART_TOKENS, MODEL_DIM), 1.0),
        'w_gate': normal_bf16(shared_keys[0], (MODEL_DIM, HIDDEN_DIM), d_std),
        'w_up': normal_bf16(shared_keys[1], (MODEL_DIM, HIDDEN_DIM), d_std),
        'w_down': normal_bf16(shared_keys[2], (HIDDEN_DIM, MODEL_DIM), f_std),
        'a_gate': normal_bf16(shared_keys[3], (NUM_ADAPTERS, MODEL_DIM, LORA_RANK), d_std),
        'b_gate': normal_bf16(shared_keys[4], (NUM_ADAPTERS, LORA_RANK, HIDDEN_DIM), b_std),
        'a_up': normal_bf16(shared_keys[5], (NUM_ADAPTERS, MODEL_DIM, LORA_RANK), d_std),
        'b_up': normal_bf16(shared_keys[6], (NUM_ADAPTERS, LORA_RANK, HIDDEN_DIM), b_std),
        'a_down': normal_bf16(shared_keys[7], (NUM_ADAPTERS, HIDDEN_DIM, LORA_RANK), f_std),
        'b_down': normal_bf16(shared_keys[8], (NUM_ADAPTERS, LORA_RANK, MODEL_DIM), b_std),
    }


def bf16_cast(values):
    return values.astype(jnp.bfloat16).astype(jnp.float32)


def reference(x, adapter_id, dout, w_gate, w_up, w_down, a_gate, b_gate, a_up, b_up, a_down, b_down):
    gate_wt = w_gate.astype(jnp.float32)
    up_wt = w_up.astype(jnp.float32)
    down_wt = w_down.astype(jnp.float32)
    model_width = x.shape[1]
    num_blocks = x.shape[0] // BLOCK_ROWS

    def block_step(grad_sums, block_in):
        x_blk, id_blk, dy_blk = block_in
        x_rows = x_blk.astype(jnp.float32)
        dy_rows = dy_blk.astype(jnp.float32)
        ag_rows = a_gate[id_blk].astype(jnp.float32)
        bg_rows = b_gate[id_blk].astype(jnp.float32)
        au_rows = a_up[id_blk].astype(jnp.float32)
        bu_rows = b_up[id_blk].astype(jnp.float32)
        ad_rows = a_down[id_blk].astype(jnp.float32)
        bd_rows = b_down[id_blk].astype(jnp.float32)
        p_gate = bf16_cast(jnp.einsum('td,tdr->tr', x_rows, ag_rows))
        p_up = bf16_cast(jnp.einsum('td,tdr->tr', x_rows, au_rows))
        e_gate = bf16_cast(LORA_SCALE * jnp.einsum('tr,trf->tf', p_gate, bg_rows))
        e_up = bf16_cast(LORA_SCALE * jnp.einsum('tr,trf->tf', p_up, bu_rows))
        gate_pre = jnp.dot(x_rows, gate_wt) + e_gate
        up_pre = jnp.dot(x_rows, up_wt) + e_up
        gate_sig = jax.nn.sigmoid(gate_pre)
        gate_act = gate_pre * gate_sig
        hidden = bf16_cast(gate_act * up_pre)
        p_down = bf16_cast(jnp.einsum('tf,tfr->tr', hidden, ad_rows))
        e_down = bf16_cast(LORA_SCALE * jnp.einsum('tr,trd->td', p_down, bd_rows))
        out_blk = (x_rows + jnp.dot(hidden, down_wt) + e_down).astype(jnp.bfloat16)
        q_down = bf16_cast(LORA_SCALE * jnp.einsum('td,trd->tr', dy_rows, bd_rows))
        dh_lora = bf16_cast(jnp.einsum('tr,tfr->tf', q_down, ad_rows))
        d_hidden = jnp.einsum('td,fd->tf', dy_rows, down_wt) + dh_lora
        d_gate = bf16_cast(d_hidden * up_pre * gate_sig * (1.0 + gate_pre * (1.0 - gate_sig)))
        d_up = bf16_cast(d_hidden * gate_act)
        q_gate = bf16_cast(LORA_SCALE * jnp.einsum('tf,trf->tr', d_gate, bg_rows))
        q_up = bf16_cast(LORA_SCALE * jnp.einsum('tf,trf->tr', d_up, bu_rows))
        dx_lora = bf16_cast(jnp.einsum('tr,tdr->td', q_gate, ag_rows) + jnp.einsum('tr,tdr->td', q_up, au_rows))
        dx_blk = (dy_rows + jnp.einsum('tf,df->td', d_gate, gate_wt) + jnp.einsum('tf,df->td', d_up, up_wt) + dx_lora).astype(jnp.bfloat16)
        updates = (
            jnp.einsum('td,tr->tdr', x_rows, q_gate),
            LORA_SCALE * jnp.einsum('tr,tf->trf', p_gate, d_gate),
            jnp.einsum('td,tr->tdr', x_rows, q_up),
            LORA_SCALE * jnp.einsum('tr,tf->trf', p_up, d_up),
            jnp.einsum('tf,tr->tfr', hidden, q_down),
            LORA_SCALE * jnp.einsum('tr,td->trd', p_down, dy_rows),
        )
        new_sums = tuple(grad_acc.at[id_blk].add(grad_upd) for grad_acc, grad_upd in zip(grad_sums, updates))
        return new_sums, (out_blk, dx_blk)

    init_sums = tuple(jnp.zeros(weight.shape, jnp.float32) for weight in (a_gate, b_gate, a_up, b_up, a_down, b_down))
    blocks_in = (
        x.reshape(num_blocks, BLOCK_ROWS, model_width),
        adapter_id.reshape(num_blocks, BLOCK_ROWS),
        dout.reshape(num_blocks, BLOCK_ROWS, model_width),
    )
    grad_sums, (out_rows, dx_rows) = lax.scan(block_step, init_sums, blocks_in)
    return (out_rows.reshape(-1, model_width), dx_rows.reshape(-1, model_width), grad_sums[0], grad_sums[1], grad_sums[2], grad_sums[3], grad_sums[4], grad_sums[5])
```

```python
import functools

import jax
import jax.numpy as jnp
from jax import lax
from jax.experimental import pallas as pl
from jax.experimental.pallas import tpu as pltpu
from jax.sharding import PartitionSpec as P


ALPHA = 32
CORE_SWAP = [(0, 1), (1, 0), (2, 3), (3, 2)]
CHIP_SWAP = [(0, 2), (2, 0), (1, 3), (3, 1)]
F32, BF16 = jnp.float32, jnp.bfloat16


VMEM_BYTES = 64000 * 1024
SHORT = 216


def dot_nn(a, b):
    return lax.dot_general(a, b, (((1,), (0,)), ((), ())), preferred_element_type=F32)


def dot_nt(a, b):
    return lax.dot_general(a, b, (((1,), (1,)), ((), ())), preferred_element_type=F32)


def call(kernel, grid, in_specs, out_specs, out_shape, scratch, flops, nbytes, aliases={}):
    return pl.pallas_call(
        kernel,
        grid_spec=pltpu.PrefetchScalarGridSpec(
            num_scalar_prefetch=1, grid=grid, in_specs=in_specs, out_specs=out_specs, scratch_shapes=scratch),
        out_shape=out_shape,
        input_output_aliases=aliases,
        compiler_params=pltpu.CompilerParams(
            dimension_semantics=('arbitrary',) * len(grid), vmem_limit_bytes=VMEM_BYTES),
        cost_estimate=pl.CostEstimate(flops=int(flops), bytes_accessed=int(nbytes), transcendentals=0),
    )


def both_forms(info_ref, section, body):
    @pl.when(info_ref[2] == 1)
    def _():
        body(SHORT)

    @pl.when(info_ref[2] == 0)
    def _():
        body(section)


def turned(tile, off):
    parts = [tile[off:2 * off], tile[:off]]
    if 2 * off < tile.shape[0]:
        parts.append(tile[2 * off:])
    return jnp.concatenate(parts, axis=0)


def pack_kernel(factor, width, rank, n_mat, info_ref, local_ref, ids_ref, r0_ref, r1_ref, r2_ref, r3_ref, *refs):
    mats, (packed_ref, p_ref, turned_ref, pt_ref, turned_t_ref, acc, sel) = refs[:n_mat], refs[n_mat:]
    step = pl.program_id(0)
    slots = packed_ref.shape[0]
    section = slots // 2

    @pl.when(step == 0)
    def _():
        acc[...] = jnp.zeros_like(acc)
        row = lax.broadcasted_iota(jnp.int32, (section, section), 0)
        for a in range(2):
            sel[a] = jnp.where(row == local_ref[a:a + 1, :], 1.0, 0.0).astype(BF16)

    mine = dot_nn(sel[0], jnp.concatenate([r0_ref[...], r1_ref[...]], axis=0))
    sib = dot_nn(sel[1], jnp.concatenate([r2_ref[...], r3_ref[...]], axis=0))

    def place(off):
        parts = [mine[:off], sib[:off]]
        if off < section:
            parts.append(jnp.zeros((slots - 2 * off, mine.shape[1]), F32))
        packed_ref[...] = jnp.concatenate(parts, axis=0).astype(BF16)

    both_forms(info_ref, section, place)
    v = packed_ref[...]
    for k, mat in enumerate(mats):
        acc[:, k * width:(k + 1) * width] += dot_nt(v, mat[...])

    @pl.when(step == pl.num_programs(0) - 1)
    def _():
        owner = ids_ref[...] - info_ref[0] * (width // rank)
        col = lax.broadcasted_iota(jnp.int32, (slots, width), 1) // rank
        keep = owner == col
        for k in range(n_mat):
            cols = slice(k * width, (k + 1) * width)
            acc[:, cols] = jnp.where(keep, acc[:, cols] * factor, 0.0)
        p_ref[...] = acc[...].astype(BF16)
        pt_ref[...] = acc[...].T.astype(BF16)

        def emit(off):
            other = turned(acc[...], off)
            turned_ref[...] = other.astype(BF16)
            turned_t_ref[...] = other.T.astype(BF16)

        both_forms(info_ref, section, emit)


def dh_kernel(info_ref, dy_ref, wd_ref, qo_ref, qs_ref, ado_ref, ads_ref, dh_ref):
    def body(off):
        m = 2 * off
        eh = (dot_nn(qo_ref[:m], ado_ref[...]) + dot_nn(qs_ref[:m], ads_ref[...])).astype(BF16)
        dh_ref[:m] = dot_nt(dy_ref[:m], wd_ref[...]) + eh.astype(F32)

    both_forms(info_ref, dy_ref.shape[0] // 2, body)


def hidden_kernel(scale, width, info_ref, x_ref, dh_ref, wg_ref, wu_ref, po_ref, ps_ref,
                  bgo_ref, bgs_ref, buo_ref, bus_ref, ado_ref, ads_ref, pt_ref, qt_ref,
                  h3_ref, qo_ref, qs_ref, gbg_ref, gbu_ref, gad_ref):
    step = pl.program_id(0)
    slots = x_ref.shape[0]

    @pl.when(step == 0)
    def _():
        qo_ref[...] = jnp.zeros_like(qo_ref)
        qs_ref[...] = jnp.zeros_like(qs_ref)

    def body(off):
        m = 2 * off

        def rank_side(k, o_ref, s_ref):
            cols = slice(k * width, (k + 1) * width)
            return dot_nn(po_ref[:m, cols], o_ref[...]) + dot_nn(ps_ref[:m, cols], s_ref[...])

        eg = (scale * rank_side(0, bgo_ref, bgs_ref)).astype(BF16)
        eu = (scale * rank_side(1, buo_ref, bus_ref)).astype(BF16)
        gate = dot_nn(x_ref[:m], wg_ref[...]) + eg.astype(F32)
        up = dot_nn(x_ref[:m], wu_ref[...]) + eu.astype(F32)
        dh = dh_ref[:m]
        sig = jax.nn.sigmoid(gate)
        act = gate * sig
        h = (act * up).astype(BF16)
        dg = (dh * up * sig * (1.0 + gate * (1.0 - sig))).astype(BF16)
        du = (dh * act).astype(BF16)
        for k, (val, o_ref, s_ref) in enumerate(((h, ado_ref, ads_ref), (dg, bgo_ref, bgs_ref), (du, buo_ref, bus_ref))):
            cols = slice(k * width, (k + 1) * width)
            h3_ref[k, :m] = val
            if m < slots:
                h3_ref[k, m:] = jnp.zeros((slots - m, val.shape[1]), BF16)
            qo_ref[:m, cols] += dot_nt(val, o_ref[...])
            qs_ref[:m, cols] += dot_nt(val, s_ref[...])

        @pl.when(step == pl.num_programs(0) - 1)
        def _():
            qs_ref[...] = turned(qs_ref[...], off)

    both_forms(info_ref, slots // 2, body)
    wide_grads(scale, width, h3_ref, pt_ref, qt_ref, gbg_ref, gbu_ref, gad_ref)


def wide_grads(scale, width, v_ref, pt_ref, qt_ref, gbg_ref, gbu_ref, gad_ref):
    gbg_ref[...] = scale * dot_nn(pt_ref[:width, :], v_ref[1])
    gbu_ref[...] = scale * dot_nn(pt_ref[width:, :], v_ref[2])
    gad_ref[...] = dot_nn(qt_ref[...], v_ref[0])


def rank_kernel(scale, width, rank, info_ref, ids_ref, own_ref, got_ref, q_ref, qt_ref):
    owner = ids_ref[...] - info_ref[0] * (width // rank)
    keep = owner == lax.broadcasted_iota(jnp.int32, (own_ref.shape[0], width), 1) // rank
    for k in range(3):
        cols = slice(k * width, (k + 1) * width)
        total = own_ref[:, cols] + got_ref[:, cols]
        total = jnp.where(keep, total * scale if k else total, 0.0)
        q_ref[:, cols] = total.astype(BF16)
        qt_ref[cols, :] = total.T.astype(BF16)


def finish_kernel(info_ref, local_ref, mine_ref, got_ref, base_ref, near_ref, far_ref):
    section = mine_ref.shape[0]
    val = (base_ref[...].astype(F32) + mine_ref[...] + got_ref[...]).astype(BF16)
    sel = jnp.where(local_ref[...] == lax.broadcasted_iota(jnp.int32, (section, section), 1), 1.0, 0.0).astype(BF16)
    rows = dot_nn(sel, val).astype(BF16)
    near_ref[...] = rows[:section // 2]
    far_ref[...] = rows[section // 2:]


def split_store(tile, off, mine_ref, sib_ref):
    mine_ref[:off] = tile[:off]
    sib_ref[:off] = tile[off:]
    if off < mine_ref.shape[0]:
        rest = jnp.zeros((mine_ref.shape[0] - off, tile.shape[1]), F32)
        mine_ref[off:] = rest
        sib_ref[off:] = rest


def dx_kernel(width, info_ref, dg_ref, du_ref, wg_ref, wu_ref, q_ref, ag_ref, au_ref, mine_ref, sib_ref):
    def body(off):
        m = 2 * off
        lora = (dot_nn(q_ref[:m, width:2 * width], ag_ref[...]) + dot_nn(q_ref[:m, 2 * width:], au_ref[...])).astype(BF16)
        tile = dot_nt(dg_ref[0, :m], wg_ref[...]) + dot_nt(du_ref[0, :m], wu_ref[...]) + lora.astype(F32)
        split_store(tile, off, mine_ref, sib_ref)

    both_forms(info_ref, mine_ref.shape[0], body)


def out_kernel(scale, width, info_ref, h_ref, wd_ref, q_ref, bd_ref, mine_ref, sib_ref):
    def body(off):
        m = 2 * off
        lora = (scale * dot_nn(q_ref[:m, :width], bd_ref[...])).astype(BF16)
        tile = dot_nn(h_ref[0, :m], wd_ref[...]) + lora.astype(F32)
        split_store(tile, off, mine_ref, sib_ref)

    both_forms(info_ref, mine_ref.shape[0], body)


def wide_grad_kernel(scale, width, info_ref, v_ref, pt_ref, qt_ref, gbg_in, gbu_in, gad_in, gbg_ref, gbu_ref, gad_ref):
    wide_grads(scale, width, v_ref, pt_ref, qt_ref, gbg_ref, gbu_ref, gad_ref)


def model_grad_kernel(scale, width, info_ref, x_ref, d_ref, qt_ref, gbd_ref, gag_ref, gau_ref):
    gbd_ref[...] = scale * dot_nn(qt_ref[:width, :], d_ref[...])
    gag_ref[...] = dot_nn(qt_ref[width:2 * width, :], x_ref[...])
    gau_ref[...] = dot_nn(qt_ref[2 * width:, :], x_ref[...])


def solution(mesh):
    tok_spec = P(('rep', 'data'), None)
    id_spec = P(('rep', 'data'))
    full_spec = P(None, None)
    own_spec = P('data', None, None)
    grad_spec = P(('rep', 'data'), None, None)

    def layer(x_loc, ids_loc, dy_loc, w_gate, w_up, w_down, a_gate, b_gate, a_up, b_up, a_down, b_down):
        toks, dim = x_loc.shape
        hid = w_gate.shape[1]
        n_local, rank = a_gate.shape[0], a_gate.shape[2]
        width = n_local * rank
        scale = ALPHA / rank
        fh = hid // 2
        section = 2 * toks
        slots = 2 * section
        me = lax.axis_index('data')
        core = me % 2
        chip = me // 2
        tie = lax.optimization_barrier

        def core_swap(v):
            return lax.ppermute(v, 'data', CORE_SWAP)

        def chip_swap(v):
            return lax.ppermute(v, 'data', CHIP_SWAP)

        ag = a_gate.transpose(0, 2, 1).reshape(width, dim)
        au = a_up.transpose(0, 2, 1).reshape(width, dim)
        bd = b_down.reshape(width, dim)
        bg = b_gate.reshape(width, hid)
        bu = b_up.reshape(width, hid)
        ad = a_down.transpose(0, 2, 1).reshape(width, hid)

        ids_mine = jnp.concatenate([ids_loc, chip_swap(ids_loc)])
        dy_send, ids_mine = tie((dy_loc, ids_mine))
        dy1 = chip_swap(dy_send)
        dy2, x2 = core_swap(dy_send), core_swap(x_loc)
        late_core, x2 = tie((core, x2))
        ids = jnp.concatenate([ids_mine, core_swap(ids_mine)])
        here = (ids // (2 * n_local) == chip).reshape(2, section)
        before = jnp.arange(section)[:, None] <= jnp.arange(section)[None, :]
        ends = jnp.dot(here.astype(F32), before.astype(F32)).astype(jnp.int32)
        short = jnp.max(ends) <= SHORT if SHORT < section else jnp.bool_(False)
        local = jnp.where(here, ends - 1, -1)
        place = local + jnp.where(short, SHORT, section) * jnp.arange(2, dtype=jnp.int32)[:, None]
        slot = jnp.where(here, place, -1).reshape(slots)
        hit = slot[None, :] == jnp.arange(slots, dtype=jnp.int32)[:, None]
        ids_slot = jnp.sum(jnp.where(hit, ids[None, :] + 1, 0), axis=1, dtype=jnp.int32) - 1
        info = jnp.stack([me, core, short.astype(jnp.int32)]).astype(jnp.int32)

        def for_sibling(v):
            return core_swap(lax.dynamic_slice_in_dim(v, (1 - late_core) * fh, fh, 1))

        ad_s, bg_s, bu_s = for_sibling(ad), for_sibling(bg), for_sibling(bu)
        dy1, ad_s, bg_s, bu_s, local, ids_slot, info = tie((dy1, ad_s, bg_s, bu_s, local, ids_slot, info))
        x_send, dy1 = tie((x_loc, dy1))
        x1 = chip_swap(x_send)
        dy3 = core_swap(dy1)

        one = dict(pipeline_mode=pl.Buffered(1))
        kt = 1024
        const = lambda *shape: pl.BlockSpec(shape, lambda i, s: (0,) * len(shape))
        vec = lambda r: pl.BlockSpec((r, kt), lambda i, s: (0, i))

        def pack(factor, rows, mats):
            n = len(mats)
            return call(
                functools.partial(pack_kernel, factor, width, rank, n), (dim // kt,),
                [const(2, section), const(slots, 1)] + [vec(toks)] * 4 + [vec(width)] * n,
                [vec(slots)] + [const(slots, n * width)] * 2 + [const(n * width, slots)] * 2,
                [jax.ShapeDtypeStruct((slots, dim), BF16)] + [jax.ShapeDtypeStruct((slots, n * width), BF16)] * 2
                + [jax.ShapeDtypeStruct((n * width, slots), BF16)] * 2,
                [pltpu.VMEM((slots, n * width), F32), pltpu.VMEM((2, section, section), BF16)],
                slots * dim * slots + 2 * n * slots * width * dim, 4 * slots * dim,
            )(info, local, ids_slot[:, None], *rows, *mats)

        dc, q_own, q_turned, qt_own, qt_turned = pack(scale, (dy_loc, dy1, dy2, dy3), (bd,))
        const1 = lambda *shape: pl.BlockSpec(shape, lambda i, s: (0,) * len(shape), **one)

        def tiles(ft):
            nf = fh // ft
            return (nf, pl.BlockSpec((width, ft), lambda i, s: (0, s[1] * nf + i)), pl.BlockSpec((width, ft), lambda i, s: (0, i)),
                    pl.BlockSpec((dim, ft), lambda i, s: (0, s[1] * nf + i)), pl.BlockSpec((ft, dim), lambda i, s: (s[1] * nf + i, 0)))

        ft = 768
        nf, own_tile, sib_tile, w_col, w_row = tiles(ft)
        dh = call(
            dh_kernel, (nf,),
            [const1(slots, dim), w_row, const1(slots, width), const1(slots, width), own_tile, sib_tile],
            pl.BlockSpec((slots, ft), lambda i, s: (0, i)), jax.ShapeDtypeStruct((slots, fh), F32),
            [], 2 * slots * dim * fh * 1.2, 2 * dim * fh,
        )(info, dc, w_down, q_own, core_swap(q_turned), ad, ad_s)
        x1, dh = tie((x1, dh))
        x3 = core_swap(x1)
        xc, p_own, p_turned, pt_own, pt_turned = pack(1.0, (x_loc, x1, x2, x3), (ag, au))
        ft = 256
        nf, own_tile, sib_tile, w_col, w_row = tiles(ft)
        g_out = pl.BlockSpec((width, ft), lambda i, s: (0, s[1] * nf + i))
        h3, qo, qs, gbg, gbu, gad = call(
            functools.partial(hidden_kernel, scale, width), (nf,),
            [const1(slots, dim), pl.BlockSpec((slots, ft), lambda i, s: (0, i)), w_col, w_col,
             const1(slots, 2 * width), const1(slots, 2 * width),
             own_tile, sib_tile, own_tile, sib_tile, own_tile, sib_tile, const1(2 * width, slots), const1(width, slots)],
            [pl.BlockSpec((3, slots, ft), lambda i, s: (0, 0, i)), const(slots, 3 * width), const(slots, 3 * width)] + [g_out] * 3,
            [jax.ShapeDtypeStruct((3, slots, fh), BF16)] + [jax.ShapeDtypeStruct((slots, 3 * width), F32)] * 2
            + [jax.ShapeDtypeStruct((width, hid), F32)] * 3,
            [], 4 * slots * dim * fh * 1.2, 4 * dim * fh,
        )(info, xc, dh, w_gate, w_up, p_own, core_swap(p_turned), bg, bg_s, bu, bu_s, ad, ad_s, pt_own, qt_own)

        q, qt = call(
            functools.partial(rank_kernel, scale, width, rank), (1,),
            [const(slots, 1), const(slots, 3 * width), const(slots, 3 * width)],
            [const(slots, 3 * width), const(3 * width, slots)],
            [jax.ShapeDtypeStruct((slots, 3 * width), BF16), jax.ShapeDtypeStruct((3 * width, slots), BF16)], [],
            1000000, 12 * slots * width,
        )(info, ids_slot[:, None], qo, core_swap(qs))
        h3_late, q = tie((h3, q))
        h3_rec = core_swap(h3_late)

        dt = 512
        q_spec = const1(slots, 3 * width)

        def plane(k):
            return pl.BlockSpec((1, slots, fh), lambda j, s: (k, 0, 0), **one)

        def dx_side(info):
            w_spec = pl.BlockSpec((dt, fh), lambda j, s: (j, s[1]))
            l_spec = pl.BlockSpec((width, dt), lambda j, s: (0, j))
            o_spec = pl.BlockSpec((section, dt), lambda j, s: (0, j))
            return call(
                functools.partial(dx_kernel, width), (dim // dt,),
                [plane(1), plane(2), w_spec, w_spec, q_spec, l_spec, l_spec], [o_spec, o_spec],
                [jax.ShapeDtypeStruct((section, dim), F32)] * 2, [],
                4 * slots * dim * fh, 4 * dim * fh,
            )(info, h3, h3, w_gate, w_up, q, ag, au)

        def out_side(info, first, count):
            w_spec = pl.BlockSpec((fh, dt), lambda j, s: (s[1], first + j))
            l_spec = pl.BlockSpec((width, dt), lambda j, s: (0, first + j))
            o_spec = pl.BlockSpec((section, dt), lambda j, s: (0, j))
            return call(
                functools.partial(out_kernel, scale, width), (count,),
                [plane(0), w_spec, q_spec, l_spec], [o_spec, o_spec],
                [jax.ShapeDtypeStruct((section, count * dt), F32)] * 2, [],
                2 * slots * count * dt * fh, 2 * count * dt * fh,
            )(info, h3, w_down, q, bd)

        def finish(mine, got, base, first):
            ct = 1280
            wide = mine.shape[1]
            cols = lambda r: pl.BlockSpec((r, ct), lambda i, s: (0, i))
            return call(
                finish_kernel, (wide // ct,),
                [const(section, 1), cols(section), cols(section), pl.BlockSpec((section, ct), lambda i, s: (0, first // ct + i))],
                [cols(toks), cols(toks)],
                [jax.ShapeDtypeStruct((toks, wide), BF16)] * 2, [],
                2 * section * section * wide, 12 * section * wide,
            )(info, local[0][:, None], mine, got, base)

        n_out = dim // dt // 2
        cut = n_out * dt
        dx_mine, dx_sib = dx_side(info)
        info_a, dx_sib = tie((info, dx_sib))
        dx_got = core_swap(dx_sib)
        a_mine, a_sib = out_side(info_a, 0, n_out)
        dx_got, a_sib = tie((dx_got, a_sib))
        dx_near, dx_far = finish(dx_mine, dx_got, dc, 0)
        a_got = core_swap(a_sib)
        info_b, dx_far = tie((info, dx_far))
        dx_back = chip_swap(dx_far)
        b_mine, b_sib = out_side(info_b, n_out, n_out)
        a_got, b_sib = tie((a_got, b_sib))
        a_near, a_far = finish(a_mine, a_got, xc, 0)
        b_got = core_swap(b_sib)
        info_c, a_far = tie((info, a_far))
        a_back = chip_swap(a_far)

        mt = 640
        m_spec = lambda r: pl.BlockSpec((r, mt), lambda i, s: (0, i))
        gbd, gag, gau = call(
            functools.partial(model_grad_kernel, scale, width), (dim // mt,),
            [m_spec(slots)] * 2 + [const(3 * width, slots)], [m_spec(width)] * 3,
            [jax.ShapeDtypeStruct((width, dim), F32)] * 3, [],
            6 * slots * width * dim, 12 * width * dim,
        )(info_c, xc, dc, qt)
        b_got, gbd = tie((b_got, gbd))
        b_near, b_far = finish(b_mine, b_got, xc, cut)
        info_d, b_far = tie((info, b_far))
        b_back = chip_swap(b_far)

        gt = 768
        n_half = fh // gt
        g_rest = pl.BlockSpec((width, gt), lambda i, s: (0, (1 - s[1]) * n_half + i))
        gbg, gbu, gad = call(
            functools.partial(wide_grad_kernel, scale, width), (n_half,),
            [pl.BlockSpec((3, slots, gt), lambda i, s: (0, 0, i)), const(2 * width, slots), const(width, slots)]
            + [pl.BlockSpec(memory_space=pl.ANY)] * 3,
            [g_rest] * 3, [jax.ShapeDtypeStruct((width, hid), F32)] * 3, [],
            6 * slots * width * fh, 12 * width * fh, {4: 0, 5: 1, 6: 2},
        )(info_d, h3_rec, pt_turned, qt_turned, gbg, gbu, gad)

        dx_back, a_back, b_back, gbg = tie((dx_back, a_back, b_back, gbg))
        home = (ids_loc // (2 * n_local) == chip)[:, None]
        dx_loc = jnp.where(home, dx_near, dx_back)
        out_loc = jnp.concatenate([jnp.where(home, a_near, a_back), jnp.where(home, b_near, b_back)], 1)

        def rows_last(v, wide):
            return v.reshape(n_local, rank, wide).transpose(0, 2, 1)

        return (out_loc, dx_loc, rows_last(gag, dim), gbg.reshape(n_local, rank, hid), rows_last(gau, dim),
                gbu.reshape(n_local, rank, hid), rows_last(gad, hid), gbd.reshape(n_local, rank, dim))

    return jax.shard_map(
        layer,
        mesh=mesh,
        in_specs=(tok_spec, id_spec, tok_spec, full_spec, full_spec, full_spec, own_spec, own_spec, own_spec, own_spec, own_spec, own_spec),
        out_specs=(tok_spec, tok_spec, grad_spec, grad_spec, grad_spec, grad_spec, grad_spec, grad_spec),
        check_vma=False,
    )
```

```python
import functools

import jax
import jax.numpy as jnp
from jax import lax
from jax.experimental import pallas as pl
from jax.experimental.pallas import tpu as pltpu
from jax.sharding import PartitionSpec as P


ALPHA = 32
CORE_SWAP = [(0, 1), (1, 0), (2, 3), (3, 2)]
CHIP_SWAP = [(0, 2), (2, 0), (1, 3), (3, 1)]
F32, BF16 = jnp.float32, jnp.bfloat16


VMEM_BYTES = 64000 * 1024
SHORT = 216


def dot_nn(a, b):
    return lax.dot_general(a, b, (((1,), (0,)), ((), ())), preferred_element_type=F32)


def dot_nt(a, b):
    return lax.dot_general(a, b, (((1,), (1,)), ((), ())), preferred_element_type=F32)


def call(kernel, grid, in_specs, out_specs, out_shape, scratch, flops, nbytes, aliases={}):
    return pl.pallas_call(
        kernel,
        grid_spec=pltpu.PrefetchScalarGridSpec(
            num_scalar_prefetch=1, grid=grid, in_specs=in_specs, out_specs=out_specs, scratch_shapes=scratch),
        out_shape=out_shape,
        input_output_aliases=aliases,
        compiler_params=pltpu.CompilerParams(
            dimension_semantics=('arbitrary',) * len(grid), vmem_limit_bytes=VMEM_BYTES),
        cost_estimate=pl.CostEstimate(flops=int(flops), bytes_accessed=int(nbytes), transcendentals=0),
    )


def both_forms(info_ref, section, body):
    @pl.when(info_ref[2] == 1)
    def _():
        body(SHORT)

    @pl.when(info_ref[2] == 0)
    def _():
        body(section)


def turned(tile, off):
    parts = [tile[off:2 * off], tile[:off]]
    if 2 * off < tile.shape[0]:
        parts.append(tile[2 * off:])
    return jnp.concatenate(parts, axis=0)


def pack_kernel(factor, width, rank, n_mat, info_ref, local_ref, ids_ref, r0_ref, r1_ref, r2_ref, r3_ref, *refs):
    mats, (packed_ref, p_ref, turned_ref, pt_ref, turned_t_ref, acc, sel) = refs[:n_mat], refs[n_mat:]
    step = pl.program_id(0)
    slots = packed_ref.shape[0]
    section = slots // 2

    @pl.when(step == 0)
    def _():
        acc[...] = jnp.zeros_like(acc)
        row = lax.broadcasted_iota(jnp.int32, (section, section), 0)
        for a in range(2):
            sel[a] = jnp.where(row == local_ref[a:a + 1, :], 1.0, 0.0).astype(BF16)

    mine = dot_nn(sel[0], jnp.concatenate([r0_ref[...], r1_ref[...]], axis=0))
    sib = dot_nn(sel[1], jnp.concatenate([r2_ref[...], r3_ref[...]], axis=0))

    def place(off):
        parts = [mine[:off], sib[:off]]
        if off < section:
            parts.append(jnp.zeros((slots - 2 * off, mine.shape[1]), F32))
        packed_ref[...] = jnp.concatenate(parts, axis=0).astype(BF16)

    both_forms(info_ref, section, place)
    v = packed_ref[...]
    for k, mat in enumerate(mats):
        acc[:, k * width:(k + 1) * width] += dot_nt(v, mat[...])

    @pl.when(step == pl.num_programs(0) - 1)
    def _():
        owner = ids_ref[...] - info_ref[0] * (width // rank)
        col = lax.broadcasted_iota(jnp.int32, (slots, width), 1) // rank
        keep = owner == col
        for k in range(n_mat):
            cols = slice(k * width, (k + 1) * width)
            acc[:, cols] = jnp.where(keep, acc[:, cols] * factor, 0.0)
        p_ref[...] = acc[...].astype(BF16)
        pt_ref[...] = acc[...].T.astype(BF16)

        def emit(off):
            other = turned(acc[...], off)
            turned_ref[...] = other.astype(BF16)
            turned_t_ref[...] = other.T.astype(BF16)

        both_forms(info_ref, section, emit)


def dh_kernel(info_ref, dy_ref, wd_ref, qo_ref, qs_ref, ado_ref, ads_ref, dh_ref):
    def body(off):
        m = 2 * off
        ranks = jnp.concatenate([qo_ref[:m], qs_ref[:m]], axis=1)
        eh = dot_nn(ranks, jnp.concatenate([ado_ref[...], ads_ref[...]], axis=0)).astype(BF16)
        dh_ref[:m] = dot_nt(dy_ref[:m], wd_ref[...]) + eh.astype(F32)

    both_forms(info_ref, dy_ref.shape[0] // 2, body)


def hidden_kernel(scale, width, info_ref, x_ref, dh_ref, wg_ref, wu_ref, po_ref, ps_ref,
                  bgo_ref, bgs_ref, buo_ref, bus_ref, ado_ref, ads_ref, pt_ref, qt_ref,
                  h3_ref, qo_ref, qs_ref, gbg_ref, gbu_ref, gad_ref):
    step = pl.program_id(0)
    slots = x_ref.shape[0]

    @pl.when(step == 0)
    def _():
        qo_ref[...] = jnp.zeros_like(qo_ref)
        qs_ref[...] = jnp.zeros_like(qs_ref)

    def body(off):
        m = 2 * off

        def both(a, b, axis):
            return jnp.concatenate([a[...], b[...]], axis=axis)

        def rank_side(k, o_ref, s_ref):
            cols = slice(k * width, (k + 1) * width)
            return dot_nn(both(po_ref[:m, cols], ps_ref[:m, cols], 1), both(o_ref, s_ref, 0))

        eg = (scale * rank_side(0, bgo_ref, bgs_ref)).astype(BF16)
        eu = (scale * rank_side(1, buo_ref, bus_ref)).astype(BF16)
        gate = dot_nn(x_ref[:m], wg_ref[...]) + eg.astype(F32)
        up = dot_nn(x_ref[:m], wu_ref[...]) + eu.astype(F32)
        dh = dh_ref[:m]
        sig = jax.nn.sigmoid(gate)
        act = gate * sig
        h = (act * up).astype(BF16)
        dg = (dh * up * sig * (1.0 + gate * (1.0 - sig))).astype(BF16)
        du = (dh * act).astype(BF16)
        values = []
        for k, (val, o_ref, s_ref) in enumerate(((h, ado_ref, ads_ref), (dg, bgo_ref, bgs_ref), (du, buo_ref, bus_ref))):
            cols = slice(k * width, (k + 1) * width)
            full = val
            if m < slots:
                full = jnp.concatenate([val, jnp.zeros((slots - m, val.shape[1]), BF16)], axis=0)
            h3_ref[k] = full
            values.append(full)
            sums = dot_nt(val, both(o_ref, s_ref, 0))
            qo_ref[:m, cols] += sums[:, :width]
            qs_ref[:m, cols] += sums[:, width:]
        wide_grads(scale, width, values, pt_ref, qt_ref, gbg_ref, gbu_ref, gad_ref)

        @pl.when(step == pl.num_programs(0) - 1)
        def _():
            qs_ref[...] = turned(qs_ref[...], off)

    both_forms(info_ref, slots // 2, body)


def wide_grads(scale, width, values, pt_ref, qt_ref, gbg_ref, gbu_ref, gad_ref):
    h, dg, du = values
    gbg_ref[...] = scale * dot_nn(pt_ref[:width, :], dg)
    gbu_ref[...] = scale * dot_nn(pt_ref[width:, :], du)
    gad_ref[...] = dot_nn(qt_ref[...], h)


def rank_kernel(scale, width, rank, info_ref, ids_ref, own_ref, got_ref, q_ref, qt_ref):
    owner = ids_ref[...] - info_ref[0] * (width // rank)
    keep = owner == lax.broadcasted_iota(jnp.int32, (own_ref.shape[0], width), 1) // rank
    factor = jnp.where(pl.program_id(0) == 0, 1.0, scale)
    total = jnp.where(keep, (own_ref[...] + got_ref[...]) * factor, 0.0)
    q_ref[...] = total.astype(BF16)
    qt_ref[...] = total.T.astype(BF16)


def finish_kernel(info_ref, local_ref, mine_ref, got_ref, base_ref, near_ref, far_ref):
    section = mine_ref.shape[0]
    val = (base_ref[...].astype(F32) + mine_ref[...] + got_ref[...]).astype(BF16)
    sel = jnp.where(local_ref[...] == lax.broadcasted_iota(jnp.int32, (section, section), 1), 1.0, 0.0).astype(BF16)
    rows = dot_nn(sel, val).astype(BF16)
    near_ref[...] = rows[:section // 2]
    far_ref[...] = rows[section // 2:]


def split_store(tile, off, mine_ref, sib_ref):
    mine_ref[:off] = tile[:off]
    sib_ref[:off] = tile[off:]
    if off < mine_ref.shape[0]:
        rest = jnp.zeros((mine_ref.shape[0] - off, tile.shape[1]), F32)
        mine_ref[off:] = rest
        sib_ref[off:] = rest


def dx_kernel(scale, width, info_ref, dg_ref, du_ref, wg_ref, wu_ref, q_ref, ag_ref, au_ref, qt_ref, x_ref, d_ref,
              mine_ref, sib_ref, gbd_ref, gag_ref, gau_ref):
    def body(off):
        gbd_ref[...] = scale * dot_nn(qt_ref[:width, :], d_ref[...])
        gag_ref[...] = dot_nn(qt_ref[width:2 * width, :], x_ref[...])
        gau_ref[...] = dot_nn(qt_ref[2 * width:, :], x_ref[...])
        m = 2 * off
        lora = (dot_nn(q_ref[:m, width:2 * width], ag_ref[...]) + dot_nn(q_ref[:m, 2 * width:], au_ref[...])).astype(BF16)
        tile = dot_nt(dg_ref[0, :m], wg_ref[...]) + dot_nt(du_ref[0, :m], wu_ref[...]) + lora.astype(F32)
        split_store(tile, off, mine_ref, sib_ref)

    both_forms(info_ref, mine_ref.shape[0], body)


def out_kernel(scale, width, info_ref, h_ref, wd_ref, q_ref, bd_ref, mine_ref, sib_ref):
    def body(off):
        m = 2 * off
        lora = (scale * dot_nn(q_ref[:m, :width], bd_ref[...])).astype(BF16)
        tile = dot_nn(h_ref[0, :m], wd_ref[...]) + lora.astype(F32)
        split_store(tile, off, mine_ref, sib_ref)

    both_forms(info_ref, mine_ref.shape[0], body)


def wide_grad_kernel(scale, width, info_ref, v_ref, pt_ref, qt_ref, gbg_in, gbu_in, gad_in, gbg_ref, gbu_ref, gad_ref):
    wide_grads(scale, width, (v_ref[0], v_ref[1], v_ref[2]), pt_ref, qt_ref, gbg_ref, gbu_ref, gad_ref)


def solution(mesh):
    tok_spec = P(('rep', 'data'), None)
    id_spec = P(('rep', 'data'))
    full_spec = P(None, None)
    own_spec = P('data', None, None)
    grad_spec = P(('rep', 'data'), None, None)

    def layer(x_loc, ids_loc, dy_loc, w_gate, w_up, w_down, a_gate, b_gate, a_up, b_up, a_down, b_down):
        toks, dim = x_loc.shape
        hid = w_gate.shape[1]
        n_local, rank = a_gate.shape[0], a_gate.shape[2]
        width = n_local * rank
        scale = ALPHA / rank
        fh = hid // 2
        section = 2 * toks
        slots = 2 * section
        me = lax.axis_index('data')
        core = me % 2
        chip = me // 2
        tie = lax.optimization_barrier

        def core_swap(v):
            return lax.ppermute(v, 'data', CORE_SWAP)

        def chip_swap(v):
            return lax.ppermute(v, 'data', CHIP_SWAP)

        ag = a_gate.transpose(0, 2, 1).reshape(width, dim)
        au = a_up.transpose(0, 2, 1).reshape(width, dim)
        bd = b_down.reshape(width, dim)
        bg = b_gate.reshape(width, hid)
        bu = b_up.reshape(width, hid)
        ad = a_down.transpose(0, 2, 1).reshape(width, hid)

        ids_mine = jnp.concatenate([ids_loc, chip_swap(ids_loc)])
        dy1 = chip_swap(dy_loc)
        dy2, x2 = core_swap(dy_loc), core_swap(x_loc)
        late_core, x2 = tie((core, x2))
        ids = jnp.concatenate([ids_mine, core_swap(ids_mine)])
        here = (ids // (2 * n_local) == chip).reshape(2, section)
        before = jnp.arange(section)[:, None] <= jnp.arange(section)[None, :]
        ends = jnp.dot(here.astype(F32), before.astype(F32)).astype(jnp.int32)
        short = jnp.max(ends) <= SHORT if SHORT < section else jnp.bool_(False)
        local = jnp.where(here, ends - 1, -1)
        place = local + jnp.where(short, SHORT, section) * jnp.arange(2, dtype=jnp.int32)[:, None]
        slot = jnp.where(here, place, -1).reshape(slots)
        hit = slot[None, :] == jnp.arange(slots, dtype=jnp.int32)[:, None]
        ids_slot = jnp.sum(jnp.where(hit, ids[None, :] + 1, 0), axis=1, dtype=jnp.int32) - 1
        info = jnp.stack([me, core, short.astype(jnp.int32)]).astype(jnp.int32)

        def for_sibling(v):
            return core_swap(lax.dynamic_slice_in_dim(v, (1 - late_core) * fh, fh, 1))

        ad_s, bg_s, bu_s = for_sibling(ad), for_sibling(bg), for_sibling(bu)
        dy1, ad_s, bg_s, bu_s, local, ids_slot, info = tie((dy1, ad_s, bg_s, bu_s, local, ids_slot, info))
        x_send, dy1 = tie((x_loc, dy1))
        x1 = chip_swap(x_send)
        dy3 = core_swap(dy1)

        one = dict(pipeline_mode=pl.Buffered(1))
        kt = 1280
        const = lambda *shape: pl.BlockSpec(shape, lambda i, s: (0,) * len(shape))
        vec = lambda r: pl.BlockSpec((r, kt), lambda i, s: (0, i))

        def pack(factor, rows, mats):
            n = len(mats)
            return call(
                functools.partial(pack_kernel, factor, width, rank, n), (dim // kt,),
                [const(2, section), const(slots, 1)] + [vec(toks)] * 4 + [vec(width)] * n,
                [vec(slots)] + [const(slots, n * width)] * 2 + [const(n * width, slots)] * 2,
                [jax.ShapeDtypeStruct((slots, dim), BF16)] + [jax.ShapeDtypeStruct((slots, n * width), BF16)] * 2
                + [jax.ShapeDtypeStruct((n * width, slots), BF16)] * 2,
                [pltpu.VMEM((slots, n * width), F32), pltpu.VMEM((2, section, section), BF16)],
                slots * dim * slots + 2 * n * slots * width * dim, 4 * slots * dim,
            )(info, local, ids_slot[:, None], *rows, *mats)

        dc, q_own, q_turned, qt_own, qt_turned = pack(scale, (dy_loc, dy1, dy2, dy3), (bd,))
        const1 = lambda *shape: pl.BlockSpec(shape, lambda i, s: (0,) * len(shape), **one)

        def tiles(ft):
            nf = fh // ft
            return (nf, pl.BlockSpec((width, ft), lambda i, s: (0, s[1] * nf + i)), pl.BlockSpec((width, ft), lambda i, s: (0, i)),
                    pl.BlockSpec((dim, ft), lambda i, s: (0, s[1] * nf + i)), pl.BlockSpec((ft, dim), lambda i, s: (s[1] * nf + i, 0)))

        ft = 768
        nf, own_tile, sib_tile, w_col, w_row = tiles(ft)
        dh = call(
            dh_kernel, (nf,),
            [const1(slots, dim), w_row, const1(slots, width), const1(slots, width), own_tile, sib_tile],
            pl.BlockSpec((slots, ft), lambda i, s: (0, i)), jax.ShapeDtypeStruct((slots, fh), F32),
            [], 2 * slots * dim * fh * 1.2, 2 * dim * fh,
        )(info, dc, w_down, q_own, core_swap(q_turned), ad, ad_s)
        x1, dh = tie((x1, dh))
        x3 = core_swap(x1)
        xc, p_own, p_turned, pt_own, pt_turned = pack(1.0, (x_loc, x1, x2, x3), (ag, au))
        ft = 256
        nf, own_tile, sib_tile, w_col, w_row = tiles(ft)
        g_out = pl.BlockSpec((width, ft), lambda i, s: (0, s[1] * nf + i))
        h3, qo, qs, gbg, gbu, gad = call(
            functools.partial(hidden_kernel, scale, width), (nf,),
            [const1(slots, dim), pl.BlockSpec((slots, ft), lambda i, s: (0, i)), w_col, w_col,
             const1(slots, 2 * width), const1(slots, 2 * width),
             own_tile, sib_tile, own_tile, sib_tile, own_tile, sib_tile, const1(2 * width, slots), const1(width, slots)],
            [pl.BlockSpec((3, slots, ft), lambda i, s: (0, 0, i)), const(slots, 3 * width), const(slots, 3 * width)] + [g_out] * 3,
            [jax.ShapeDtypeStruct((3, slots, fh), BF16)] + [jax.ShapeDtypeStruct((slots, 3 * width), F32)] * 2
            + [jax.ShapeDtypeStruct((width, hid), F32)] * 3,
            [], 4 * slots * dim * fh * 1.2, 4 * dim * fh,
        )(info, xc, dh, w_gate, w_up, p_own, core_swap(p_turned), bg, bg_s, bu, bu_s, ad, ad_s, pt_own, qt_own)

        third = pl.BlockSpec((slots, width), lambda i, s: (0, i))
        q, qt = call(
            functools.partial(rank_kernel, scale, width, rank), (3,),
            [const(slots, 1), third, third], [third, pl.BlockSpec((width, slots), lambda i, s: (i, 0))],
            [jax.ShapeDtypeStruct((slots, 3 * width), BF16), jax.ShapeDtypeStruct((3 * width, slots), BF16)], [],
            1000000, 12 * slots * width,
        )(info, ids_slot[:, None], qo, core_swap(qs))
        h3_late, q = tie((h3, q))
        h3_rec = core_swap(h3_late)

        dt = 512
        q_spec = const1(slots, 3 * width)

        def plane(k):
            return pl.BlockSpec((1, slots, fh), lambda j, s: (k, 0, 0), **one)

        def dx_side(info):
            nt = 256
            w_spec = pl.BlockSpec((nt, fh), lambda j, s: (j, s[1]))
            tile = lambda r: pl.BlockSpec((r, nt), lambda j, s: (0, j))
            return call(
                functools.partial(dx_kernel, scale, width), (dim // nt,),
                [plane(1), plane(2), w_spec, w_spec, q_spec, tile(width), tile(width), const1(3 * width, slots), tile(slots), tile(slots)],
                [tile(section)] * 2 + [tile(width)] * 3,
                [jax.ShapeDtypeStruct((section, dim), F32)] * 2 + [jax.ShapeDtypeStruct((width, dim), F32)] * 3, [],
                4 * slots * dim * fh, 4 * dim * fh,
            )(info, h3, h3, w_gate, w_up, q, ag, au, qt, xc, dc)

        def out_side(info, first, count):
            w_spec = pl.BlockSpec((fh, dt), lambda j, s: (s[1], first + j))
            l_spec = pl.BlockSpec((width, dt), lambda j, s: (0, first + j))
            o_spec = pl.BlockSpec((section, dt), lambda j, s: (0, j))
            return call(
                functools.partial(out_kernel, scale, width), (count,),
                [plane(0), w_spec, q_spec, l_spec], [o_spec, o_spec],
                [jax.ShapeDtypeStruct((section, count * dt), F32)] * 2, [],
                2 * slots * count * dt * fh, 2 * count * dt * fh,
            )(info, h3, w_down, q, bd)

        def finish(mine, got, base, first):
            ct = 1280
            wide = mine.shape[1]
            cols = lambda r: pl.BlockSpec((r, ct), lambda i, s: (0, i))
            return call(
                finish_kernel, (wide // ct,),
                [const(section, 1), cols(section), cols(section), pl.BlockSpec((section, ct), lambda i, s: (0, first // ct + i))],
                [cols(toks), cols(toks)],
                [jax.ShapeDtypeStruct((toks, wide), BF16)] * 2, [],
                2 * section * section * wide, 12 * section * wide,
            )(info, local[0][:, None], mine, got, base)

        n_out = dim // dt // 2
        cut = n_out * dt
        dx_mine, dx_sib, gbd, gag, gau = dx_side(info)
        info_a, dx_sib = tie((info, dx_sib))
        dx_got = core_swap(dx_sib)
        a_mine, a_sib = out_side(info_a, 0, n_out)
        dx_got, a_sib = tie((dx_got, a_sib))
        dx_near, dx_far = finish(dx_mine, dx_got, dc, 0)
        a_got = core_swap(a_sib)
        info_b, dx_far = tie((info, dx_far))
        dx_back = chip_swap(dx_far)
        b_mine, b_sib = out_side(info_b, n_out, n_out)
        a_got, b_sib = tie((a_got, b_sib))
        a_near, a_far = finish(a_mine, a_got, xc, 0)
        b_got = core_swap(b_sib)
        a_back = chip_swap(a_far)
        b_got, a_far = tie((b_got, a_far))
        b_near, b_far = finish(b_mine, b_got, xc, cut)
        info_d, b_far = tie((info, b_far))
        b_back = chip_swap(b_far)

        gt = 1152
        n_half = fh // gt
        g_rest = pl.BlockSpec((width, gt), lambda i, s: (0, (1 - s[1]) * n_half + i))
        gbg, gbu, gad = call(
            functools.partial(wide_grad_kernel, scale, width), (n_half,),
            [pl.BlockSpec((3, slots, gt), lambda i, s: (0, 0, i)), const(2 * width, slots), const(width, slots)]
            + [pl.BlockSpec(memory_space=pl.ANY)] * 3,
            [g_rest] * 3, [jax.ShapeDtypeStruct((width, hid), F32)] * 3, [],
            6 * slots * width * fh, 12 * width * fh, {4: 0, 5: 1, 6: 2},
        )(info_d, h3_rec, pt_turned, qt_turned, gbg, gbu, gad)

        dx_back, a_back, b_back, gbg = tie((dx_back, a_back, b_back, gbg))
        home = (ids_loc // (2 * n_local) == chip)[:, None]
        dx_loc = jnp.where(home, dx_near, dx_back)
        out_loc = jnp.concatenate([jnp.where(home, a_near, a_back), jnp.where(home, b_near, b_back)], 1)

        def rows_last(v, wide):
            return v.reshape(n_local, rank, wide).transpose(0, 2, 1)

        return (out_loc, dx_loc, rows_last(gag, dim), gbg.reshape(n_local, rank, hid), rows_last(gau, dim),
                gbu.reshape(n_local, rank, hid), rows_last(gad, hid), gbd.reshape(n_local, rank, dim))

    return jax.shard_map(
        layer,
        mesh=mesh,
        in_specs=(tok_spec, id_spec, tok_spec, full_spec, full_spec, full_spec, own_spec, own_spec, own_spec, own_spec, own_spec, own_spec),
        out_specs=(tok_spec, tok_spec, grad_spec, grad_spec, grad_spec, grad_spec, grad_spec, grad_spec),
        check_vma=False,
    )
```
